32 devices in a mesh: dp: 1 (over z), tp: 4 (over y), cp: 8 (over x, core).
Axes of the slice: x: 4, y: 4, z: 1, core: 2. Of those that a mesh axis runs over, the one named last changes fastest.
The devices are a block of a 4x4x8 slice.
Arguments:
- hidden: bfloat16 [6, 3072, 2304], P('dp', 'cp')
- cotangent: bfloat16 [6, 3072, 2304], P('dp', 'cp')
- positions: int32 [3072], P(('dp', 'cp'))
- w_q: bfloat16 [2304, 2048], P(None, 'tp')
- w_k: bfloat16 [2304, 1024], P(None, 'tp')
- w_v: bfloat16 [2304, 1024], P(None, 'tp')
- w_o: bfloat16 [2048, 2304], P('tp')
- w_pre: float32 [2304], replicated
- w_post: float32 [2304], replicated
- q_norm: float32 [256], replicated
- k_norm: float32 [256], replicated
Outputs:
- output 1: bfloat16 [6, 3072, 2304], P('dp', 'cp')
- output 2: bfloat16 [6, 3072, 2304], P('dp', 'cp')
- output 3: float32 [2304, 2048], P('dp', 'tp')
- output 4: float32 [2304, 1024], P('dp', 'tp')
- output 5: float32 [2304, 1024], P('dp', 'tp')
- output 6: float32 [2048, 2304], P(('dp', 'tp'))
- output 7: float32 [2304], P('dp')
- output 8: float32 [2304], P('dp')
- output 9: float32 [256], P('dp')
- output 10: float32 [256], P('dp')
All inputs are finite; a program needn't handle non-finite values.
Results may differ from the reference program's by a relative error of at most 0.02.
Values are sent between devices in bfloat16 or wider.
A program may use at most 768 MiB of HBM per device.

```python
import jax
import jax.numpy as jnp
from jax import lax

BATCH = 6
SEQ_LEN = 3072
MODEL_DIM = 2304
NUM_HEADS = 8
KV_HEADS = 4
HEAD_DIM = 256
CP_SIZE = 8
QUERY_BLOCK = 64
POS_RANGE = 131072

EPS = 1e-6
ROPE_BASE = 1000000.0
ROPE_SCALE = 8.0
NEG_BIG = -1e30


def draw_positions(key):
    gap_max = POS_RANGE // SEQ_LEN
    pos_gaps = jax.random.randint(key, (SEQ_LEN,), 1, gap_max + 1, dtype=jnp.int32)
    logical = jnp.cumsum(pos_gaps) - pos_gaps[0]
    piece_len = SEQ_LEN // (2 * CP_SIZE)
    pieces = logical.reshape(2 * CP_SIZE, piece_len)
    layout = jnp.stack([pieces[:CP_SIZE], pieces[CP_SIZE:][::-1]], axis=1)
    return layout.reshape(SEQ_LEN).astype(jnp.int32)


def setup_inputs(seed: int = 0, part: int = 0) -> dict:
    part_keys = jax.random.split(jax.random.fold_in(jax.random.key(seed), part), 3)
    weight_keys = jax.random.split(jax.random.key(seed + 1), 8)
    act_shape = (BATCH, SEQ_LEN, MODEL_DIM)
    q_cols = NUM_HEADS * HEAD_DIM
    kv_cols = KV_HEADS * HEAD_DIM
    hidden = jax.random.normal(part_keys[0], act_shape, jnp.float32).astype(jnp.bfloat16)
    cotangent = jax.random.normal(part_keys[1], act_shape, jnp.float32).astype(jnp.bfloat16)
    w_q = (jax.random.normal(weight_keys[0], (MODEL_DIM, q_cols), jnp.float32) * MODEL_DIM ** -0.5).astype(jnp.bfloat16)
    w_k = (jax.random.normal(weight_keys[1], (MODEL_DIM, kv_cols), jnp.float32) * MODEL_DIM ** -0.5).astype(jnp.bfloat16)
    w_v = (jax.random.normal(weight_keys[2], (MODEL_DIM, kv_cols), jnp.float32) * MODEL_DIM ** -0.5).astype(jnp.bfloat16)
    w_o = (jax.random.normal(weight_keys[3], (q_cols, MODEL_DIM), jnp.float32) * q_cols ** -0.5).astype(jnp.bfloat16)
    w_pre = 0.3 * jax.random.normal(weight_keys[4], (MODEL_DIM,), jnp.float32)
    w_post = 0.3 * jax.random.normal(weight_keys[5], (MODEL_DIM,), jnp.float32)
    q_norm = 0.3 * jax.random.normal(weight_keys[6], (HEAD_DIM,), jnp.float32)
    k_norm = 0.3 * jax.random.normal(weight_keys[7], (HEAD_DIM,), jnp.float32)
    return {'hidden': hidden, 'cotangent': cotangent, 'positions': draw_positions(part_keys[2]), 'w_q': w_q, 'w_k': w_k, 'w_v': w_v, 'w_o': w_o, 'w_pre': w_pre, 'w_post': w_post, 'q_norm': q_norm, 'k_norm': k_norm}


def rms_unit(values):
    return values * lax.rsqrt(jnp.mean(values * values, axis=-1, keepdims=True) + EPS)


def to_bf16(values):
    return values.astype(jnp.bfloat16).astype(jnp.float32)


def rope_apply(values, cos_t, sin_t):
    half_dim = values.shape[-1] // 2
    lower_half = values[..., :half_dim]
    upper_half = values[..., half_dim:]
    return jnp.concatenate([lower_half * cos_t - upper_half * sin_t, upper_half * cos_t + lower_half * sin_t], axis=-1)


def block_forward(x_f32, w_q, w_k, w_v, w_o, w_pre, w_post, q_norm, k_norm, positions):
    groups = NUM_HEADS // KV_HEADS
    normed = to_bf16(rms_unit(x_f32) * (1.0 + w_pre))
    q_raw = to_bf16(jnp.einsum('bsd,dh->bsh', normed, w_q)).reshape(BATCH, SEQ_LEN, NUM_HEADS, HEAD_DIM)
    k_raw = to_bf16(jnp.einsum('bsd,dh->bsh', normed, w_k)).reshape(BATCH, SEQ_LEN, KV_HEADS, HEAD_DIM)
    v_heads = to_bf16(jnp.einsum('bsd,dh->bsh', normed, w_v)).reshape(BATCH, SEQ_LEN, KV_HEADS, HEAD_DIM)
    half_dim = HEAD_DIM // 2
    inv_freq = 1.0 / (ROPE_SCALE * ROPE_BASE ** (jnp.arange(half_dim, dtype=jnp.float32) * (2.0 / HEAD_DIM)))
    angles = positions.astype(jnp.float32)[:, None] * inv_freq[None, :]
    cos_t = jnp.cos(angles)[None, :, None, :]
    sin_t = jnp.sin(angles)[None, :, None, :]
    q_fin = to_bf16(rope_apply(rms_unit(q_raw) * (1.0 + q_norm), cos_t, sin_t))
    k_fin = to_bf16(rope_apply(rms_unit(k_raw) * (1.0 + k_norm), cos_t, sin_t))
    score_scale = HEAD_DIM ** -0.5
    n_blocks = SEQ_LEN // QUERY_BLOCK
    q_blocks = jnp.moveaxis(q_fin.reshape(BATCH, n_blocks, QUERY_BLOCK, KV_HEADS, groups, HEAD_DIM), 1, 0)
    pos_blocks = positions.reshape(n_blocks, QUERY_BLOCK)

    def one_block(block_in):
        q_blk, q_pos = block_in
        scores = jnp.einsum('bqkgd,bskd->bkgqs', q_blk, k_fin) * score_scale
        allowed = positions[None, :] <= q_pos[:, None]
        attn_prob = jax.nn.softmax(jnp.where(allowed, scores, NEG_BIG), axis=-1)
        return jnp.einsum('bkgqs,bskd->bqkgd', attn_prob, v_heads)

    block_outs = lax.map(jax.checkpoint(one_block), (q_blocks, pos_blocks))
    attn_in = to_bf16(jnp.moveaxis(block_outs, 0, 1).reshape(BATCH, SEQ_LEN, NUM_HEADS * HEAD_DIM))
    attn = jnp.einsum('bsh,hd->bsd', attn_in, w_o)
    return x_f32 + rms_unit(attn) * (1.0 + w_post)


def reference(hidden, cotangent, positions, w_q, w_k, w_v, w_o, w_pre, w_post, q_norm, k_norm):
    def forward(x_f32, wq_f32, wk_f32, wv_f32, wo_f32, pre_gain, post_gain, q_gain, k_gain):
        return block_forward(x_f32, wq_f32, wk_f32, wv_f32, wo_f32, pre_gain, post_gain, q_gain, k_gain, positions)

    out_f32, pullback = jax.vjp(forward, hidden.astype(jnp.float32), w_q.astype(jnp.float32), w_k.astype(jnp.float32), w_v.astype(jnp.float32), w_o.astype(jnp.float32), w_pre, w_post, q_norm, k_norm)
    grad_list = pullback(cotangent.astype(jnp.float32))
    return (out_f32.astype(jnp.bfloat16), grad_list[0].astype(jnp.bfloat16), grad_list[1], grad_list[2], grad_list[3], grad_list[4], grad_list[5], grad_list[6], grad_list[7], grad_list[8])
```

```python
import functools
import math

import jax
import jax.numpy as jnp
from jax import lax
from jax.experimental import pallas as pl
from jax.experimental.pallas import tpu as pltpu
from jax.sharding import Mesh, PartitionSpec as P


EPS = 1e-6
ROPE_BASE = 1000000.0
ROPE_SCALE = 8.0
NEG_BIG = -1e30
LOG2E = math.log2(math.e)
VMEM_LIMIT = 60 * 1024 * 1024
BF = jnp.bfloat16
F32 = jnp.float32


def dot_nn(a, b):
    return lax.dot_general(a, b, (((1,), (0,)), ((), ())), preferred_element_type=F32)


def dot_nt(a, b):
    return lax.dot_general(a, b, (((1,), (1,)), ((), ())), preferred_element_type=F32)


def rms_inv(values):
    return lax.rsqrt(jnp.mean(values * values, axis=-1, keepdims=True) + EPS)


def rope_apply(values, cos_t, sin_t):
    half = values.shape[-1] // 2
    lo, hi = values[:, :half], values[:, half:]
    return jnp.concatenate([lo * cos_t - hi * sin_t, hi * cos_t + lo * sin_t], axis=-1)


def rope_back(values, cos_t, sin_t):
    half = values.shape[-1] // 2
    lo, hi = values[:, :half], values[:, half:]
    return jnp.concatenate([lo * cos_t + hi * sin_t, hi * cos_t - lo * sin_t], axis=-1)


def head_norm(raw_bf, gain, cos_t, sin_t):
    raw = raw_bf.astype(F32)
    return rope_apply(raw * rms_inv(raw) * (1.0 + gain), cos_t, sin_t).astype(BF)


def head_norm_back(grad, raw_bf, gain, cos_t, sin_t):
    raw = raw_bf.astype(F32)
    inv = rms_inv(raw)
    unit = raw * inv
    d_scaled = rope_back(grad, cos_t, sin_t)
    d_gain = jnp.sum(d_scaled * unit, axis=0, keepdims=True)
    d_unit = d_scaled * (1.0 + gain)
    d_raw = inv * (d_unit - unit * jnp.mean(d_unit * unit, axis=-1, keepdims=True))
    return d_raw.astype(BF), d_gain


def pre_body(x_ref, wq_ref, wk_ref, wv_ref, pre_ref, qg_ref, kg_ref, cos_ref, sin_ref, normed_ref, qraw_ref, kraw_ref, qfin_ref, kv_ref):
    hd = qg_ref.shape[1]
    x = x_ref[0].astype(F32)
    n = (x * rms_inv(x) * (1.0 + pre_ref[...])).astype(BF)
    normed_ref[0] = n
    cos_t, sin_t = cos_ref[...], sin_ref[...]
    kraw = dot_nn(n, wk_ref[...]).astype(BF)
    kraw_ref[0] = kraw
    kv_ref[0, :, :hd] = head_norm(kraw, kg_ref[...], cos_t, sin_t)
    kv_ref[0, :, hd:] = dot_nn(n, wv_ref[...]).astype(BF)
    qraw = dot_nn(n, wq_ref[...]).astype(BF)
    qraw_ref[0] = qraw
    for h in range(qraw.shape[1] // hd):
        cols = slice(h * hd, (h + 1) * hd)
        qfin_ref[0, :, cols] = head_norm(qraw[:, cols], qg_ref[...], cos_t, sin_t)


def const_spec(shape):
    return pl.BlockSpec(shape, lambda *_: (0,) * len(shape), pipeline_mode=pl.Buffered(1))


def params(sem=("arbitrary",)):
    return pltpu.CompilerParams(dimension_semantics=sem, vmem_limit_bytes=VMEM_LIMIT)


def pre_call(off, nb, hidden, w_q, w_k, w_v, w_pre, q_norm, k_norm, cos_t, sin_t):
    _, s, d = hidden.shape
    dq, dk = w_q.shape[1], w_k.shape[1]
    row = lambda width: pl.BlockSpec((1, s, width), lambda b: (b, 0, 0))
    shape = lambda width: jax.ShapeDtypeStruct((nb, s, width), BF)
    return pl.pallas_call(
        pre_body,
        grid=(nb,),
        in_specs=[pl.BlockSpec((1, s, d), lambda b: (b + off, 0, 0)), const_spec(w_q.shape), const_spec(w_k.shape), const_spec(w_v.shape), const_spec(w_pre.shape), const_spec(q_norm.shape), const_spec(k_norm.shape), const_spec(cos_t.shape), const_spec(sin_t.shape)],
        out_specs=[row(d), row(dq), row(dk), row(dq), row(2 * dk)],
        out_shape=[shape(d), shape(dq), shape(dk), shape(dq), shape(2 * dk)],
        compiler_params=params(),
        cost_estimate=pl.CostEstimate(flops=2 * nb * s * d * (dq + 2 * dk), bytes_accessed=4 * nb * s * d, transcendentals=0),
        name="pre",
    )(hidden, w_q, w_k, w_v, w_pre, q_norm, k_norm, cos_t, sin_t)


def seq_copies(src, buf, sem, b, slot, piece):
    owners = src.shape[0]
    out = []
    for o in range(owners):
        for half, p in ((0, o), (1, 2 * owners - 1 - o)):
            out.append(pltpu.make_async_copy(src.at[o, b, pl.ds(half * piece, piece)], buf.at[slot, pl.ds(p * piece, piece)], sem.at[slot]))
    return out


def stream(pairs, b, nb, piece):
    slot = lax.rem(b, 2)

    @pl.when(b == 0)
    def _():
        for src, buf, sem in pairs:
            for cp in seq_copies(src, buf, sem, 0, 0, piece):
                cp.start()

    for src, buf, sem in pairs:
        for cp in seq_copies(src, buf, sem, b, slot, piece):
            cp.wait()

    @pl.when(b + 1 < nb)
    def _():
        for src, buf, sem in pairs:
            for cp in seq_copies(src, buf, sem, b + 1, 1 - slot, piece):
                cp.start()

    return slot


def fwd_body(nb, owners, hd, c_ref, q_ref, kv_ref, o_ref, of_ref, lse_ref, buf, sem, acc_ref, m_ref, l_ref):
    b = pl.program_id(0)
    piece = q_ref.shape[1] // 2
    blk = 4 * piece
    heads = q_ref.shape[2] // hd
    factor = hd ** -0.5 * LOG2E
    slot = stream([(kv_ref, buf, sem)], b, nb, piece)
    c = c_ref[0]
    for half in (0, 1):
        p = c if half == 0 else 2 * owners - 1 - c
        last = p // 4
        shift = (p - 4 * last) * piece
        rows = slice(half * piece, (half + 1) * piece)

        def keys(j):
            base = pl.multiple_of(j * blk, blk)
            return buf[slot, pl.ds(base, blk), :hd], buf[slot, pl.ds(base, blk), hd:]

        k_blk, v_blk = keys(last)
        for h in range(heads):
            s2 = dot_nt(q_ref[0, rows, h * hd:(h + 1) * hd], k_blk) * factor
            gap = lax.broadcasted_iota(jnp.int32, s2.shape, 1) - lax.broadcasted_iota(jnp.int32, s2.shape, 0)
            s2 = jnp.where(gap <= shift, s2, NEG_BIG)
            m = jnp.max(s2, axis=1, keepdims=True)
            prob = jnp.exp2(s2 - m)
            m_ref[h] = m
            l_ref[h] = jnp.sum(prob, axis=1, keepdims=True)
            acc_ref[h] = dot_nn(prob.astype(BF), v_blk)

        def step(j, carry):
            k_blk, v_blk = keys(j)
            for h in range(heads):
                s2 = dot_nt(q_ref[0, rows, h * hd:(h + 1) * hd], k_blk) * factor
                m_old = m_ref[h]
                m = jnp.maximum(m_old, jnp.max(s2, axis=1, keepdims=True))
                prob = jnp.exp2(s2 - m)
                alpha = jnp.exp2(m_old - m)
                m_ref[h] = m
                l_ref[h] = l_ref[h] * alpha + jnp.sum(prob, axis=1, keepdims=True)
                acc_ref[h] = acc_ref[h] * alpha + dot_nn(prob.astype(BF), v_blk)
            return carry

        lax.fori_loop(0, last, step, 0)
        for h in range(heads):
            out = acc_ref[h] / l_ref[h]
            cols = slice(h * hd, (h + 1) * hd)
            of_ref[0, rows, cols] = out
            o_ref[0, rows, cols] = out.astype(BF)
            lse_ref[0, rows, h:h + 1] = m_ref[h] + jnp.log2(l_ref[h])


def fwd_call(c_arr, q_fin, kv_all, hd):
    nb, s, dq = q_fin.shape
    owners = kv_all.shape[0]
    heads = dq // hd
    piece = s // 2
    row = lambda width: pl.BlockSpec((1, s, width), lambda b: (b, 0, 0))
    return pl.pallas_call(
        functools.partial(fwd_body, nb, owners, hd),
        grid=(nb,),
        in_specs=[pl.BlockSpec(memory_space=pltpu.SMEM), row(dq), pl.BlockSpec(memory_space=pl.ANY)],
        out_specs=[row(dq), row(dq), row(heads)],
        out_shape=[jax.ShapeDtypeStruct((nb, s, dq), BF), jax.ShapeDtypeStruct((nb, s, dq), F32), jax.ShapeDtypeStruct((nb, s, heads), F32)],
        scratch_shapes=[pltpu.VMEM((2, owners * s, kv_all.shape[3]), BF), pltpu.SemaphoreType.DMA((2,)), pltpu.VMEM((heads, piece, hd), F32), pltpu.VMEM((heads, piece, 1), F32), pltpu.VMEM((heads, piece, 1), F32)],
        compiler_params=params(),
        cost_estimate=pl.CostEstimate(flops=2 * nb * s * owners * s * dq, bytes_accessed=2 * kv_all.size, transcendentals=nb * s * owners * s // 2),
        name="attend",
    )(c_arr, q_fin, kv_all)


def mid_body(hd, t_ref, o0_ref, o1_ref, o2_ref, o3_ref, of_ref, x_ref, gy_ref, wfull_ref, wo_ref, post_ref, *rest):
    y_ref, dattn_ref, dout_ref, delta_ref, dpost_ref, ocat_ref = rest[-6:]
    first = jnp.logical_and(pl.program_id(0) == 0, pl.program_id(1) == 0)
    dq = o0_ref.shape[2]
    for i, ref in enumerate((o0_ref, o1_ref, o2_ref, o3_ref)):
        ocat_ref[:, pl.ds(pl.multiple_of(t_ref[i] * dq, dq), dq)] = ref[0]
    attn = dot_nn(ocat_ref[...], wfull_ref[...])
    inv = rms_inv(attn)
    unit = attn * inv
    gain = 1.0 + post_ref[...]
    y_ref[0] = (x_ref[0].astype(F32) + unit * gain).astype(BF)
    gy = gy_ref[0].astype(F32)
    part = jnp.sum(gy * unit, axis=0, keepdims=True)

    @pl.when(first)
    def _():
        dpost_ref[...] = part

    @pl.when(jnp.logical_not(first))
    def _():
        dpost_ref[...] += part

    d_unit = gy * gain
    d_attn = (inv * (d_unit - unit * jnp.mean(d_unit * unit, axis=-1, keepdims=True))).astype(BF)
    dattn_ref[0] = d_attn
    d_out = dot_nt(d_attn, wo_ref[...]).astype(BF)
    dout_ref[0] = d_out
    prod = d_out.astype(F32) * of_ref[0]
    for h in range(dq // hd):
        delta_ref[0, :, h:h + 1] = jnp.sum(prod[:, h * hd:(h + 1) * hd], axis=1, keepdims=True)


def mid_call(off, nb, hd, t_arr, o_blocks, o_f32, hidden, cotangent, w_full, w_o, w_post, carried):
    batch, s, d = hidden.shape
    dq = o_f32.shape[2]
    tile = s // 2
    loc = lambda width: pl.BlockSpec((1, tile, width), lambda b, i: (b, i, 0))
    full = lambda width: pl.BlockSpec((1, tile, width), lambda b, i: (b + off, i, 0))
    ins = [t_arr, *o_blocks, o_f32, hidden, cotangent, w_full, w_o, w_post]
    in_specs = [pl.BlockSpec(memory_space=pltpu.SMEM)] + [loc(dq)] * 5 + [full(d), full(d), const_spec(w_full.shape), const_spec(w_o.shape), const_spec(w_post.shape)]
    aliases = {}
    if carried is not None:
        for i, arr in enumerate(carried):
            aliases[len(ins)] = i
            ins.append(arr)
            in_specs.append(pl.BlockSpec(memory_space=pl.ANY))
    return pl.pallas_call(
        functools.partial(mid_body, hd),
        grid=(nb, 2),
        in_specs=in_specs,
        out_specs=[full(d), full(d), loc(dq), loc(dq // hd), pl.BlockSpec((1, d), lambda b, i: (0, 0))],
        out_shape=[jax.ShapeDtypeStruct((batch, s, d), BF), jax.ShapeDtypeStruct((batch, s, d), BF), jax.ShapeDtypeStruct((nb, s, dq), BF), jax.ShapeDtypeStruct((nb, s, dq // hd), F32), jax.ShapeDtypeStruct((1, d), F32)],
        scratch_shapes=[pltpu.VMEM((tile, w_full.shape[0]), BF)],
        input_output_aliases=aliases,
        compiler_params=params(("arbitrary", "arbitrary")),
        cost_estimate=pl.CostEstimate(flops=2 * nb * s * d * (w_full.shape[0] + dq), bytes_accessed=10 * nb * s * d, transcendentals=0),
        name="mid",
    )(*ins)


def dq_body(nb, owners, hd, c_ref, q_ref, do_ref, lse_ref, delta_ref, qraw_ref, gain_ref, cos_ref, sin_ref, kv_ref, dq_ref, dgain_ref, buf, sem, acc_ref):
    b = pl.program_id(0)
    piece = q_ref.shape[1] // 2
    blk = 4 * piece
    heads = q_ref.shape[2] // hd
    scale = hd ** -0.5
    factor = scale * LOG2E
    slot = stream([(kv_ref, buf, sem)], b, nb, piece)
    c = c_ref[0]
    total = jnp.zeros((1, hd), F32)
    for half in (0, 1):
        p = c if half == 0 else 2 * owners - 1 - c
        last = p // 4
        shift = (p - 4 * last) * piece
        rows = slice(half * piece, (half + 1) * piece)

        def block(j, h, masked):
            base = pl.multiple_of(j * blk, blk)
            k_blk, v_blk = buf[slot, pl.ds(base, blk), :hd], buf[slot, pl.ds(base, blk), hd:]
            cols = slice(h * hd, (h + 1) * hd)
            s2 = dot_nt(q_ref[0, rows, cols], k_blk) * factor
            prob = jnp.exp2(s2 - lse_ref[0, rows, h:h + 1])
            if masked:
                gap = lax.broadcasted_iota(jnp.int32, s2.shape, 1) - lax.broadcasted_iota(jnp.int32, s2.shape, 0)
                prob = jnp.where(gap <= shift, prob, 0.0)
            d_prob = dot_nt(do_ref[0, rows, cols], v_blk)
            d_score = (prob * (d_prob - delta_ref[0, rows, h:h + 1]) * scale).astype(BF)
            return dot_nn(d_score, k_blk)

        for h in range(heads):
            acc_ref[h] = block(last, h, True)

        def step(j, carry):
            for h in range(heads):
                acc_ref[h] += block(j, h, False)
            return carry

        lax.fori_loop(0, last, step, 0)
        for h in range(heads):
            cols = slice(h * hd, (h + 1) * hd)
            d_raw, d_gain = head_norm_back(acc_ref[h], qraw_ref[0, rows, cols], gain_ref[...], cos_ref[rows, :], sin_ref[rows, :])
            dq_ref[0, rows, cols] = d_raw
            total = total + d_gain

    @pl.when(b == 0)
    def _():
        dgain_ref[...] = total

    @pl.when(b > 0)
    def _():
        dgain_ref[...] += total


def dq_call(c_arr, q_fin, d_out, lse, delta, q_raw, q_norm, cos_t, sin_t, kv_all, hd):
    nb, s, dq = q_fin.shape
    owners = kv_all.shape[0]
    heads = dq // hd
    piece = s // 2
    row = lambda width: pl.BlockSpec((1, s, width), lambda b: (b, 0, 0))
    return pl.pallas_call(
        functools.partial(dq_body, nb, owners, hd),
        grid=(nb,),
        in_specs=[pl.BlockSpec(memory_space=pltpu.SMEM), row(dq), row(dq), row(heads), row(heads), row(dq), const_spec(q_norm.shape), const_spec(cos_t.shape), const_spec(sin_t.shape), pl.BlockSpec(memory_space=pl.ANY)],
        out_specs=[row(dq), pl.BlockSpec((1, hd), lambda b: (0, 0))],
        out_shape=[jax.ShapeDtypeStruct((nb, s, dq), BF), jax.ShapeDtypeStruct((1, hd), F32)],
        scratch_shapes=[pltpu.VMEM((2, owners * s, kv_all.shape[3]), BF), pltpu.SemaphoreType.DMA((2,)), pltpu.VMEM((heads, piece, hd), F32)],
        compiler_params=params(),
        cost_estimate=pl.CostEstimate(flops=3 * nb * s * owners * s * dq, bytes_accessed=2 * kv_all.size, transcendentals=nb * s * owners * s // 2),
        name="grad_q",
    )(c_arr, q_fin, d_out, lse, delta, q_raw, q_norm, cos_t, sin_t, kv_all)


def dkv_body(nb, owners, hd, c_ref, kv_ref, stat_ref, kraw_ref, gain_ref, cos_ref, sin_ref, q_ref, do_ref, dkv_ref, dgain_ref, qbuf, dobuf, qsem, dosem, dk_ref, dv_ref):
    b = pl.program_id(0)
    piece = kv_ref.shape[1] // 2
    blk = 4 * piece
    n_blk = 2 * owners // 4
    heads = qbuf.shape[2] // hd
    scale = hd ** -0.5
    factor = scale * LOG2E
    slot = stream([(q_ref, qbuf, qsem), (do_ref, dobuf, dosem)], b, nb, piece)
    c = c_ref[0]
    total = jnp.zeros((1, hd), F32)
    for half in (0, 1):
        p = c if half == 0 else 2 * owners - 1 - c
        first = p // 4
        shift = (p - 4 * first) * piece
        rows = slice(half * piece, (half + 1) * piece)
        k_own, v_own = kv_ref[0, rows, :hd], kv_ref[0, rows, hd:]

        def block(j, masked):
            base = pl.multiple_of(j * blk, blk)
            dk_new, dv_new = None, None
            for h in range(heads):
                cols = slice(h * hd, (h + 1) * hd)
                q_blk, do_blk = qbuf[slot, pl.ds(base, blk), cols], dobuf[slot, pl.ds(base, blk), cols]
                s2 = dot_nt(k_own, q_blk) * factor
                prob = jnp.exp2(s2 - stat_ref[0, h:h + 1, pl.ds(base, blk)])
                if masked:
                    gap = lax.broadcasted_iota(jnp.int32, s2.shape, 0) - lax.broadcasted_iota(jnp.int32, s2.shape, 1)
                    prob = jnp.where(gap <= -shift, prob, 0.0)
                d_prob = dot_nt(v_own, do_blk)
                d_score = (prob * (d_prob - stat_ref[0, heads + h:heads + h + 1, pl.ds(base, blk)]) * scale).astype(BF)
                dv_h = dot_nn(prob.astype(BF), do_blk)
                dk_h = dot_nn(d_score, q_blk)
                dk_new = dk_h if dk_new is None else dk_new + dk_h
                dv_new = dv_h if dv_new is None else dv_new + dv_h
            return dk_new, dv_new

        dk_ref[...], dv_ref[...] = block(first, True)

        def step(j, carry):
            dk_new, dv_new = block(j, False)
            dk_ref[...] += dk_new
            dv_ref[...] += dv_new
            return carry

        lax.fori_loop(first + 1, n_blk, step, 0)
        d_raw, d_gain = head_norm_back(dk_ref[...], kraw_ref[0, rows, :], gain_ref[...], cos_ref[rows, :], sin_ref[rows, :])
        dkv_ref[0, rows, :hd] = d_raw
        dkv_ref[0, rows, hd:] = dv_ref[...].astype(BF)
        total = total + d_gain

    @pl.when(b == 0)
    def _():
        dgain_ref[...] = total

    @pl.when(b > 0)
    def _():
        dgain_ref[...] += total


def dkv_call(c_arr, kv_loc, stats, k_raw, k_norm, cos_t, sin_t, q_all, do_all, hd):
    nb, s, dkv = kv_loc.shape
    owners = q_all.shape[0]
    piece = s // 2
    row = lambda width: pl.BlockSpec((1, s, width), lambda b: (b, 0, 0))
    return pl.pallas_call(
        functools.partial(dkv_body, nb, owners, hd),
        grid=(nb,),
        in_specs=[pl.BlockSpec(memory_space=pltpu.SMEM), row(dkv), pl.BlockSpec((1,) + stats.shape[1:], lambda b: (b, 0, 0)), row(hd), const_spec(k_norm.shape), const_spec(cos_t.shape), const_spec(sin_t.shape), pl.BlockSpec(memory_space=pl.ANY), pl.BlockSpec(memory_space=pl.ANY)],
        out_specs=[row(dkv), pl.BlockSpec((1, hd), lambda b: (0, 0))],
        out_shape=[jax.ShapeDtypeStruct((nb, s, dkv), BF), jax.ShapeDtypeStruct((1, hd), F32)],
        scratch_shapes=[pltpu.VMEM((2, owners * s, q_all.shape[3]), BF), pltpu.VMEM((2, owners * s, q_all.shape[3]), BF), pltpu.SemaphoreType.DMA((2,)), pltpu.SemaphoreType.DMA((2,)), pltpu.VMEM((piece, hd), F32), pltpu.VMEM((piece, hd), F32)],
        compiler_params=params(),
        cost_estimate=pl.CostEstimate(flops=4 * nb * s * owners * s * q_all.shape[3], bytes_accessed=4 * q_all.size, transcendentals=nb * s * owners * s // 2),
        name="grad_kv",
    )(c_arr, kv_loc, stats, k_raw, k_norm, cos_t, sin_t, q_all, do_all)


def shift_by(arr, axis, n, amount):
    return lax.ppermute(arr, axis, [(i, (i + amount) % n) for i in range(n)])


def ring_gather(arr, axis, n):
    half = arr.shape[0] // 2
    prev = shift_by(arr, axis, n, 1)
    nxt = shift_by(arr, axis, n, -1)
    far_a = shift_by(prev[:half], axis, n, 1)
    far_b = shift_by(nxt[half:], axis, n, -1)
    return arr, prev, nxt, jnp.concatenate([far_a, far_b], axis=0)


def ring_ids(t, n):
    return [t, (t + n - 1) % n, (t + 1) % n, (t + 2) % n]


def place(blocks, ids, n):
    out = jnp.zeros((n,) + blocks[0].shape, blocks[0].dtype)
    for blk, i in zip(blocks, ids):
        out = lax.dynamic_update_slice(out, blk[None], (i,) + (0,) * blk.ndim)
    return out


def solution(mesh):
    n_dp, n_tp, n_cp = mesh.shape['dp'], mesh.shape['tp'], mesh.shape['cp']
    assert n_tp == 4 and n_cp % 2 == 0
    fine = Mesh(mesh.devices.reshape(n_dp, n_tp, n_cp // 2, 2), ('dp', 'tp', 'cx', 'cc'))
    CP = ('cx', 'cc')

    def per_device(hidden, cotangent, pos_loc, w_q, w_k, w_v, w_o, w_pre, w_post, q_norm, k_norm):
        hd = q_norm.shape[0]
        batch, s, d = hidden.shape
        dq, dk = w_q.shape[1], w_k.shape[1]
        t = lax.axis_index('tp')
        core = lax.axis_index('cc')
        c = lax.axis_index('cx') * 2 + core
        c_arr = jnp.full((1,), c, jnp.int32)
        ids = ring_ids(t, n_tp)
        t_arr = jnp.stack(ids).astype(jnp.int32)
        nc = 3 if batch % 3 == 0 else 1
        nb = batch // nc
        w_pre2, w_post2, qg2, kg2 = w_pre[None], w_post[None], q_norm[None], k_norm[None]

        half_dim = hd // 2
        inv_freq = 1.0 / (ROPE_SCALE * ROPE_BASE ** (jnp.arange(half_dim, dtype=F32) * (2.0 / hd)))
        angles = pos_loc.astype(F32)[:, None] * inv_freq[None, :]
        cos_t, sin_t = jnp.cos(angles), jnp.sin(angles)

        def gather_weight(half):
            blocks = ring_gather(half, 'tp', n_tp)
            mine = place(blocks, ids, n_tp)
            other = lax.ppermute(mine, 'cc', [(0, 1), (1, 0)])
            return jnp.where(core == 0, mine, other), jnp.where(core == 0, other, mine)

        wo_a, wo_b = gather_weight(lax.dynamic_slice(w_o, (core * (dq // 2), 0), (dq // 2, d)))
        w_full = jnp.concatenate([wo_a, wo_b], axis=1).reshape(n_tp * dq, d)

        pre, kv_all, att = [], [], []
        for i in range(nc):
            pre.append(pre_call(i * nb, nb, hidden, w_q, w_k, w_v, w_pre2, qg2, kg2, cos_t, sin_t))
            kv_all.append(lax.all_gather(pre[i][4], CP))
            att.append(fwd_call(c_arr, pre[i][3], kv_all[i], hd))
        o_blocks = [ring_gather(att[i][0], 'tp', n_tp) for i in range(nc)]

        q_all = []
        for i in range(nc):
            q_all.append(lax.all_gather(pre[i][3], CP))

        carried, d_outs, deltas, d_posts = None, [], [], []
        for i in range(nc):
            y, d_attn, d_out, delta, d_post = mid_call(i * nb, nb, hd, t_arr, o_blocks[i], att[i][1], hidden, cotangent, w_full, w_o, w_post2, carried)
            carried = (y, d_attn)
            d_outs.append(d_out)
            deltas.append(delta)
            d_posts.append(d_post)
        output, d_attn = carried
        d_post = sum(d_posts)

        do_all = []
        for i in range(nc):
            do_all.append(lax.all_gather(d_outs[i], CP))
        heads = dq // hd

        st = jnp.concatenate([jnp.concatenate([att[i][2], deltas[i]], axis=-1) for i in range(nc)], axis=0)
        st = jnp.tile(jnp.moveaxis(st, 2, 1), (1, 4, 1))
        st = lax.all_gather(st, CP)[:, :, :2 * heads]
        st = jnp.concatenate([st[..., :s // 2], st[..., s // 2:][::-1]], axis=0)
        stats = jnp.moveaxis(st, 0, 2).reshape(batch, 2 * heads, n_cp * s)

        w_qkv_t = jnp.concatenate([w_q, w_k, w_v], axis=1).T
        half_w = lax.dynamic_slice(w_qkv_t, (core * ((dq + 2 * dk) // 2), 0), ((dq + 2 * dk) // 2, d))
        half_w = lax.optimization_barrier((half_w, o_blocks[nc - 1][3]))[0]
        wt_q, wt_kv = gather_weight(half_w)
        wt_q, wt_kv = wt_q.reshape(n_tp * dq, d), wt_kv.reshape(n_tp * 2 * dk, d)

        o_full = jnp.concatenate([att[i][0] for i in range(nc)], axis=0).reshape(batch * s, dq)
        dw_o = lax.dot_general(o_full, d_attn.reshape(batch * s, d), (((0,), (0,)), ((), ())), preferred_element_type=F32)
        dw_o = lax.psum(dw_o, CP)

        gq = []
        for i in range(nc):
            gq.append(dq_call(c_arr, pre[i][3], d_outs[i], att[i][2], deltas[i], pre[i][1], qg2, cos_t, sin_t, kv_all[i], hd))
        gkv = []
        for i in range(nc):
            gkv.append(dkv_call(c_arr, pre[i][4], stats[i * nb:(i + 1) * nb], pre[i][2], kg2, cos_t, sin_t, q_all[i], do_all[i], hd))

        normed = jnp.concatenate([pre[i][0] for i in range(nc)], axis=0).reshape(batch * s, d)
        dq_flat = jnp.concatenate([g[0] for g in gq], axis=0).reshape(batch * s, dq)
        dkv_flat = jnp.concatenate([g[0] for g in gkv], axis=0).reshape(batch * s, 2 * dk)

        def weight_grad(cot):
            return lax.dot_general(normed, cot, (((0,), (0,)), ((), ())), preferred_element_type=F32)

        dq_flat, dkv_flat, dw_o = lax.optimization_barrier((dq_flat, dkv_flat, dw_o))
        dws = (weight_grad(dq_flat), weight_grad(dkv_flat[:, :dk]), weight_grad(dkv_flat[:, dk:]))
        dw_q, dw_k, dw_v = lax.psum(dws, CP)

        rows = nb * s
        quarter = rows // n_tp
        d_hidden = jnp.zeros((batch * s, d), BF)
        x_flat, gy_flat = hidden.reshape(batch * s, d), cotangent.reshape(batch * s, d)
        d_pre = jnp.zeros((d,), F32)

        def exchange(chunk):
            blocks = chunk.reshape(n_tp, quarter, chunk.shape[-1])
            take = lambda i: lax.dynamic_index_in_dim(blocks, i, 0, keepdims=False)
            recv = [take(t)]
            for amount in (1, n_tp - 1, 2):
                recv.append(shift_by(take((t + amount) % n_tp), 'tp', n_tp, amount))
            out = place(recv, [t, (t + n_tp - 1) % n_tp, (t + 1) % n_tp, (t + 2) % n_tp], n_tp)
            return jnp.moveaxis(out, 0, 1).reshape(quarter, n_tp * chunk.shape[-1])

        for i in range(nc):
            ex_q = exchange(gq[i][0].reshape(rows, dq))
            ex_kv = exchange(gkv[i][0].reshape(rows, 2 * dk))
            d_normed = dot_nn(ex_q, wt_q) + dot_nn(ex_kv, wt_kv)
            base = i * rows + t * quarter
            x = lax.dynamic_slice(x_flat, (base, 0), (quarter, d)).astype(F32)
            gy = lax.dynamic_slice(gy_flat, (base, 0), (quarter, d)).astype(F32)
            inv = rms_inv(x)
            unit = x * inv
            d_pre = d_pre + jnp.sum(d_normed * unit, axis=0)
            d_unit = d_normed * (1.0 + w_pre)
            dx = (gy + inv * (d_unit - unit * jnp.mean(d_unit * unit, axis=-1, keepdims=True))).astype(BF)
            for blk, j in zip(ring_gather(dx, 'tp', n_tp), ids):
                d_hidden = lax.dynamic_update_slice(d_hidden, blk, (i * rows + j * quarter, 0))

        small = jnp.concatenate([d_pre, sum(g[1] for g in gq)[0], sum(g[1] for g in gkv)[0]])
        for bit in (1, 2):
            small = small + lax.ppermute(small, 'tp', [(i, i ^ bit) for i in range(n_tp)])
        small, d_post = lax.psum((small, d_post), CP)
        d_pre, d_qnorm, d_knorm = small[:d], small[d:d + hd], small[d + hd:]
        return output, d_hidden.reshape(batch, s, d), dw_q, dw_k, dw_v, dw_o, d_pre, d_post[0], d_qnorm, d_knorm

    cp = ('cx', 'cc')
    specs_in = (P('dp', cp, None), P('dp', cp, None), P(('dp',) + cp), P(None, 'tp'), P(None, 'tp'), P(None, 'tp'), P('tp', None), P(None), P(None), P(None), P(None))
    specs_out = (P('dp', cp, None), P('dp', cp, None), P('dp', 'tp'), P('dp', 'tp'), P('dp', 'tp'), P(('dp', 'tp'), None), P('dp'), P('dp'), P('dp'), P('dp'))

    return jax.shard_map(per_device, mesh=fine, in_specs=specs_in, out_specs=specs_out, check_vma=False)
```
